32 devices in a mesh: row: 4 (over z), col: 8 (over y, x, core).
Axes of the slice: x: 2, y: 2, z: 4, core: 2. Of those that a mesh axis runs over, the one named last changes fastest.
Arguments:
- points: float32 [8, 2048], P(None, ('row', 'col')), may hold values from -15 to 15
- noise_level: float32 [2048], P('row'), may hold values from 0.5 to 2
- right_sides: float32 [64, 2048], P(None, 'row'), may hold values from -6 to 6
Outputs:
- solution: float32 [64, 2048], P(None, 'row')
- residual: float32 [64, 2048], P(None, 'row')
- rel_norms: float32 [64], replicated
The draws below stay inside these ranges and needn't reach their ends.
All inputs are finite; a program needn't handle non-finite values.
Results may differ from the reference program's by a relative error of at most 0.0008.
Values sent between devices are 32-bit elements; how exact they have to be, the bound alone decides.
A program may use at most 64 MiB of HBM per device.

```python
import math
import jax
import jax.numpy as jnp
from jax import lax

DIM = 8
RHS = 64
ITERS = 2
NPTS = 2048


def block_levels(key, shape, cuts, least, largest):
    loudness, own = 1.0, jax.random.fold_in(key, 6)
    for position, shards_of in cuts:
        draws = jnp.exp(jax.random.uniform(jax.random.fold_in(own, position), (shards_of,), jnp.float32, least / len(cuts), largest / len(cuts)))
        loudness = loudness * jnp.repeat(draws, shape[position] // shards_of).reshape([-1 if axis == position else 1 for axis in range(len(shape))])
    return loudness


def centred(stream_key, shape, scale, most, pieces=(), kind=jnp.bfloat16):
    drawn = jax.random.normal(stream_key, shape, jnp.float32) * scale
    if len(pieces) > 0:
        drawn = block_levels(stream_key, shape, pieces, -0.22, 0.18) * drawn
    return jnp.clip(drawn, min=-most, max=most).astype(kind)


def setup_inputs(seed: int = 0) -> dict:
    arg_keys = jax.random.split(jax.random.key(seed), 4)
    points = centred(arg_keys[0], (DIM, NPTS), 2.5, 15.0, ((1, 32),), jnp.float32)
    noise_level = jnp.clip(jnp.exp(math.log(2.0) - 1.3862944 * jax.random.uniform(arg_keys[1], (NPTS,), jnp.float32) ** block_levels(arg_keys[1], (NPTS,), ((0, 4),), -0.2, 0.2)), 0.5, 2.0)
    right_sides = centred(arg_keys[2], (RHS, NPTS), 1.0, 6.0, ((1, 4),), jnp.float32)
    return {"points": points, "noise_level": noise_level, "right_sides": right_sides}


HIGH = lax.Precision.HIGHEST

def operate(direction, points, sq_norms, noise_level):
    total = points.shape[1]
    tile_rows = math.gcd(total, 2048)
    count = total // tile_rows

    def one_tile(index, image):
        offset = index * tile_rows
        tile_points = lax.dynamic_slice_in_dim(points, offset, tile_rows, 1)
        tile_sq = lax.dynamic_slice_in_dim(sq_norms, offset, tile_rows, 0)
        sq_dist = tile_sq[:, None] + sq_norms[None, :] - 2.0 * jnp.dot(tile_points.T, points, precision=HIGH)
        kernel = jnp.exp(-0.5 * sq_dist)
        piece = lax.dot_general(direction, kernel, (((1,), (1,)), ((), ())), precision=HIGH)
        return lax.dynamic_update_slice_in_dim(image, piece, offset, 1)
    image = lax.fori_loop(0, count, one_tile, jnp.zeros(direction.shape, jnp.float32))
    return image + noise_level[None, :] * direction

def products(first, second):
    return lax.dot_general(first, second, (((1,), (1,)), ((), ())), precision=HIGH)

def solve_sym(matrix, target):
    lower = jnp.linalg.cholesky(0.5 * (matrix + matrix.T))
    return jax.scipy.linalg.cho_solve((lower, True), target)

def reference(points, noise_level, right_sides):
    sq_norms = lax.optimization_barrier(jnp.sum(points * points, axis=0))
    solution = jnp.zeros_like(right_sides)
    residual = right_sides
    direction = right_sides
    gram = products(residual, residual)
    first = gram
    new_gram = gram
    for iteration in range(ITERS):
        image = operate(direction, points, sq_norms, noise_level)
        curv = products(direction, image)
        step_coef = solve_sym(curv, gram)
        solution = solution + jnp.dot(step_coef.T, direction, precision=HIGH)
        residual = residual - jnp.dot(step_coef.T, image, precision=HIGH)
        new_gram = products(residual, residual)
        if iteration + 1 < ITERS:
            dir_coef = solve_sym(gram, new_gram)
            direction = residual + jnp.dot(dir_coef.T, direction, precision=HIGH)
        gram = new_gram
    rel_norms = jnp.sqrt(jnp.diagonal(new_gram) / jnp.diagonal(first))
    return (solution, residual, rel_norms)
```

```python
import functools
import math

import jax
import jax.numpy as jnp
from jax import lax
from jax.experimental import pallas as pl
from jax.experimental.pallas import tpu as pltpu
from jax.sharding import PartitionSpec as P

ITERS = 2
HIGH = lax.Precision.HIGHEST
MESH = pl.DeviceIdType.MESH
F32 = jnp.float32
BF16 = jnp.bfloat16


def bdot(first, second, dims):
    return lax.dot_general(first, second, (dims, ((), ())), preferred_element_type=F32)


def fdot(first, second, dims):
    return lax.dot_general(
        first, second, (dims, ((), ())), precision=HIGH, preferred_element_type=F32
    )


NT = ((1,), (1,))
TN = ((0,), (0,))
NN = ((1,), (0,))


def split2(value):
    high = value.astype(BF16)
    return high, (value - high.astype(F32)).astype(BF16)


def split3(value):
    high = value.astype(BF16)
    rest = value - high.astype(F32)
    mid = rest.astype(BF16)
    return high, mid, (rest - mid.astype(F32)).astype(BF16)


def solve_spd(matrix, target):
    size = matrix.shape[0]
    matrix = 0.5 * (matrix + matrix.T)
    both = jnp.concatenate([target, matrix], axis=1)
    width = both.shape[1]
    base = target.shape[1]
    panels = size // 8
    tiles = [both[8 * t : 8 * t + 8] for t in range(panels)]
    sublane = lax.broadcasted_iota(jnp.int32, (8, width), 0)

    def lane(tile, j):
        return jnp.broadcast_to(tile[:, j : j + 1], (8, width))

    def row(tile, s):
        return jnp.broadcast_to(tile[s : s + 1, :], (8, width))

    for k in range(panels):
        start = base + 8 * k
        cols = [lane(tiles[k], start + j) for j in range(8)]
        others = {
            t: [lane(tiles[t], start + j) for j in range(8)]
            for t in range(panels)
            if t != k
        }
        panel = tiles[k]
        for s in range(8):
            scale = 1.0 / row(cols[s], s)
            here = sublane == s
            factor = cols[s]

            def step(value):
                pivot = row(value, s) * scale
                return jnp.where(here, pivot, value - factor * pivot)

            panel = step(panel)
            for j in range(s + 1, 8):
                cols[j] = step(cols[j])
        rows = [row(panel, s) for s in range(8)]
        tiles[k] = panel
        for t in others:
            total = others[t][0] * rows[0]
            for s in range(1, 8):
                total = total + others[t][s] * rows[s]
            tiles[t] = tiles[t] - total
    return jnp.concatenate(tiles, axis=0)[:, :base]


def kernel_body(
    n_row, n_col,
    pts_ref, noise_ref, rhs_ref,
    sol_ref, res_ref, rel_ref,
    pbuf, rbuf, nbuf, left, right, khi, klo, vst, img, dirs,
    psem, psend, nsem, nsend, zsem, zsend, csem, csend,
):
    z = lax.axis_index("row")
    c = lax.axis_index("col")
    dim, piece = pts_ref.shape
    rhs_count, block = rhs_ref.shape
    total = block * n_row
    rows = rhs_count // n_col

    barrier = pltpu.get_barrier_semaphore()
    for dz in range(1, n_row):
        pl.semaphore_signal(barrier, inc=1, device_id=(lax.rem(z + dz, n_row), c), device_id_type=MESH)
    for dc in range(1, n_col):
        pl.semaphore_signal(barrier, inc=1, device_id=(z, lax.rem(c + dc, n_col)), device_id_type=MESH)
    pl.semaphore_wait(barrier, n_row + n_col - 2)

    mine = pl.ds(pl.multiple_of(c * rows, rows), rows)
    copies = []

    def send(src, dst, ssem, rsem, device):
        copy = pltpu.make_async_remote_copy(
            src_ref=src, dst_ref=dst, send_sem=ssem, recv_sem=rsem,
            device_id=device, device_id_type=MESH,
        )
        copy.start()
        copies.append(copy)
        return copy

    p_z, r_z, n_z = [None], [None], [None]
    for dz in range(1, n_row):
        dev = (lax.rem(z + dz, n_row), c)
        p_z.append(send(pts_ref, pbuf.at[z, c], psend.at[dz, 0], psem.at[dz, 0], dev))
    for dz in range(1, n_row):
        dev = (lax.rem(z + dz, n_row), c)
        r_z.append(send(rhs_ref.at[mine, :], rbuf.at[z, mine, :], zsend.at[dz], zsem.at[dz], dev))
        n_z.append(send(noise_ref, nbuf.at[z], nsend.at[dz], nsem.at[dz], dev))
    p_c = {}
    r_c = {}
    for dc in range(1, n_col):
        dev = (z, lax.rem(c + dc, n_col))
        p_c[0, dc] = send(pts_ref, pbuf.at[z, c], psend.at[0, dc], psem.at[0, dc], dev)
    pbuf[z, c] = pts_ref[...]
    rbuf[z] = rhs_ref[...]
    nbuf[z] = noise_ref[...]
    for dz in range(1, n_row):
        src_z = lax.rem(z + n_row - dz, n_row)
        p_z[dz].wait_recv()
        for dc in range(1, n_col):
            dev = (z, lax.rem(c + dc, n_col))
            p_c[dz, dc] = send(pbuf.at[src_z, c], pbuf.at[src_z, c], psend.at[dz, dc], psem.at[dz, dc], dev)
    for dz in range(1, n_row):
        src_z = lax.rem(z + n_row - dz, n_row)
        r_z[dz].wait_recv()
        n_z[dz].wait_recv()
        for dc in range(1, n_col):
            dev = (z, lax.rem(c + dc, n_col))
            part = rbuf.at[src_z, mine, :]
            r_c[dz, dc] = send(part, part, csend.at[dz, dc], csem.at[dz, dc], dev)
    for dz in range(n_row):
        for dc in range(1, n_col):
            p_c[dz, dc].wait_recv()

    pair = 128 // piece
    for zz in range(n_row):
        for m in range(n_col // pair):
            x = jnp.concatenate([pbuf[zz, m * pair + q] for q in range(pair)], axis=1)
            half = -0.5 * jnp.sum(x * x, axis=0, keepdims=True)
            one = jnp.ones_like(half)
            pad = jnp.zeros((16 - dim - 2, pair * piece), F32)
            lh, lm, ll = split3(jnp.concatenate([x, half, one, pad], axis=0))
            rh, rm, rl = split3(jnp.concatenate([x, one, half, pad], axis=0))
            at = pl.ds(zz * block + m * pair * piece, pair * piece)
            left[:, at] = jnp.concatenate([lh, lh, lm, lh, ll, lm], axis=0)
            right[:, at] = jnp.concatenate([rh, rm, rh, rl, rh, rm], axis=0)

    tile = 256
    wide = 512

    def build(t, carry):
        at = pl.ds(pl.multiple_of(t * tile, tile), tile)
        lhs = left[:, at]
        for w in range(total // wide):
            cols = pl.ds(w * wide, wide)
            high, low = split2(jnp.exp(bdot(lhs, right[:, cols], TN)))
            khi[at, cols] = high
            klo[at, cols] = low
        return carry

    lax.fori_loop(0, total // tile, build, 0)

    for dz in range(1, n_row):
        for dc in range(1, n_col):
            r_c[dz, dc].wait_recv()

    def operate(source):
        for zz in range(n_row):
            high, low = split2(source[zz])
            vst[pl.ds(0, rhs_count), pl.ds(zz * block, block)] = high
            vst[pl.ds(rhs_count, rhs_count), pl.ds(zz * block, block)] = low
        for zz in range(n_row):
            cols = pl.ds(zz * block, block)
            main = bdot(vst[...], khi[:, cols], NN)
            minor = bdot(vst[pl.ds(0, rhs_count), :], klo[:, cols], NN)
            img[zz] = (main[:rhs_count] + (main[rhs_count:] + minor)) + nbuf[zz] * source[zz]

    def products(first, second):
        out = fdot(first[0], second[0], NT)
        for zz in range(1, n_row):
            out = out + fdot(first[zz], second[zz], NT)
        return out

    gram = products(rbuf, rbuf)
    operate(rbuf)
    coef = solve_spd(products(rbuf, img), gram)
    first_sum = jnp.zeros((8, rhs_count), F32)
    ones = jnp.ones((8, block), F32)
    my_sol = fdot(coef, rhs_ref[...], TN)
    for copy in copies:
        copy.wait_send()
    for zz in range(n_row):
        base = rbuf[zz]
        first_sum = first_sum + fdot(ones, base * base, NT)
        dirs[zz] = base
        rbuf[zz] = base - fdot(coef, img[zz], TN)
    dcoef = solve_spd(gram, products(rbuf, rbuf))
    gram = products(rbuf, rbuf)
    for zz in range(n_row):
        dirs[zz] = rbuf[zz] + fdot(dcoef, dirs[zz], TN)
    operate(dirs)
    coef = solve_spd(products(dirs, img), gram)
    sol_ref[...] = my_sol + fdot(coef, dirs[z], TN)
    last_sum = jnp.zeros((8, rhs_count), F32)
    for zz in range(n_row):
        new = rbuf[zz] - fdot(coef, img[zz], TN)
        img[zz] = new
        last_sum = last_sum + fdot(ones, new * new, NT)
    res_ref[...] = img[z]
    rel_ref[...] = jnp.sqrt(last_sum / first_sum)[0:1]


def fits(n_row, n_col, points, right_sides):
    rhs_count, block = right_sides.shape
    dim, piece = points.shape
    total = block * n_row
    return (
        rhs_count == 64
        and rhs_count % (8 * n_col) == 0
        and 128 % piece == 0
        and n_col % (128 // piece) == 0
        and total % 512 == 0
        and block % 128 == 0
        and dim <= 14
        and total * total * 4 <= 20 * 2**20
    )


def fused(points, noise_level, right_sides):
    n_row = lax.axis_size("row")
    n_col = lax.axis_size("col")
    rhs_count, block = right_sides.shape
    dim, piece = points.shape
    total = block * n_row
    vmem = pl.BlockSpec(memory_space=pltpu.VMEM)
    sol, res, rel = pl.pallas_call(
        functools.partial(kernel_body, n_row, n_col),
        out_shape=(
            jax.ShapeDtypeStruct((rhs_count, block), F32),
            jax.ShapeDtypeStruct((rhs_count, block), F32),
            jax.ShapeDtypeStruct((1, rhs_count), F32),
        ),
        in_specs=[vmem] * 3,
        out_specs=(vmem,) * 3,
        scratch_shapes=[
            pltpu.VMEM((n_row, n_col, dim, piece), F32),
            pltpu.VMEM((n_row, rhs_count, block), F32),
            pltpu.VMEM((n_row, 1, block), F32),
            pltpu.VMEM((96, total), BF16),
            pltpu.VMEM((96, total), BF16),
            pltpu.VMEM((total, total), BF16),
            pltpu.VMEM((total, total), BF16),
            pltpu.VMEM((2 * rhs_count, total), BF16),
            pltpu.VMEM((n_row, rhs_count, block), F32),
            pltpu.VMEM((n_row, rhs_count, block), F32),
            pltpu.SemaphoreType.DMA((n_row, n_col)),
            pltpu.SemaphoreType.DMA((n_row, n_col)),
            pltpu.SemaphoreType.DMA((n_row,)),
            pltpu.SemaphoreType.DMA((n_row,)),
            pltpu.SemaphoreType.DMA((n_row,)),
            pltpu.SemaphoreType.DMA((n_row,)),
            pltpu.SemaphoreType.DMA((n_row, n_col)),
            pltpu.SemaphoreType.DMA((n_row, n_col)),
        ],
        compiler_params=pltpu.CompilerParams(
            collective_id=0, has_side_effects=True, vmem_limit_bytes=60 * 2**20
        ),
    )(points, noise_level[None, :], right_sides)
    return sol, res, rel[0]


def from_root(value, axis, root):
    mine = lax.axis_index(axis) == root
    return lax.psum(jnp.where(mine, value, jnp.zeros_like(value)), axis)


def products(first, second):
    return lax.dot_general(first, second, (((1,), (1,)), ((), ())), precision=HIGH)


def solve_sym(matrix, target):
    lower = jnp.linalg.cholesky(0.5 * (matrix + matrix.T))
    return jax.scipy.linalg.cho_solve((lower, True), target)


def gram_sum(single):
    return lax.psum(single, "row")


def triple_sum(first, second, third):
    return lax.psum((first, second, third), "row")


def on_device(points, noise_level, right_sides):
    row_count = lax.axis_size("row")
    col_count = lax.axis_size("col")
    if fits(row_count, col_count, points, right_sides):
        return fused(points, noise_level, right_sides)
    row_index = lax.axis_index("row")
    col_index = lax.axis_index("col")
    pts_dev = points.shape[1]
    row_len = pts_dev * col_count
    col_len = pts_dev * row_count
    col_ratio = col_count // row_count
    all_points = lax.all_gather(points, ("row", "col"), axis=1, tiled=True)
    sq_norms = jnp.sum(all_points * all_points, axis=0)
    row_points = lax.dynamic_slice_in_dim(all_points, row_index * row_len, row_len, 1)
    row_sq = lax.dynamic_slice_in_dim(sq_norms, row_index * row_len, row_len, 0)
    col_points = lax.dynamic_slice_in_dim(all_points, col_index * col_len, col_len, 1)
    col_sq = lax.dynamic_slice_in_dim(sq_norms, col_index * col_len, col_len, 0)
    tile_rows = math.gcd(row_len, 512)
    tile_count = row_len // tile_rows
    rhs_count = right_sides.shape[0]
    residual = right_sides
    solution = jnp.zeros_like(residual)
    direction = residual
    gram = gram_sum(products(residual, residual))
    first = gram
    new_gram = gram
    for iteration in range(ITERS):
        source = lax.dynamic_slice_in_dim(direction, col_index % col_ratio * col_len, col_len, 1)
        col_direction = from_root(source, "row", col_index // col_ratio)

        def one_tile(index, result):
            offset = index * tile_rows
            tile_points = lax.dynamic_slice_in_dim(row_points, offset, tile_rows, 1)
            tile_sq = lax.dynamic_slice_in_dim(row_sq, offset, tile_rows, 0)
            sq_dist = (
                tile_sq[:, None]
                + col_sq[None, :]
                - 2.0 * jnp.dot(tile_points.T, col_points, precision=HIGH)
            )
            kernel = jnp.exp(-0.5 * sq_dist)
            return lax.dynamic_update_slice_in_dim(
                result, products(col_direction, kernel), offset, 1
            )

        image = (
            lax.psum(
                lax.fori_loop(
                    0, tile_count, one_tile, jnp.zeros((rhs_count, row_len), jnp.float32)
                ),
                "col",
            )
            + noise_level[None, :] * direction
        )
        curv, cross, image_gram = triple_sum(
            products(direction, image), products(residual, image), products(image, image)
        )
        step_coef = solve_sym(curv, gram)
        solution = solution + jnp.dot(step_coef.T, direction, precision=HIGH)
        residual = residual - jnp.dot(step_coef.T, image, precision=HIGH)
        cross_coef = jnp.dot(cross, step_coef, precision=HIGH)
        quad = jnp.dot(step_coef.T, jnp.dot(image_gram, step_coef, precision=HIGH), precision=HIGH)
        new_gram = gram - cross_coef - cross_coef.T + quad
        if iteration + 1 < ITERS:
            dir_coef = solve_sym(gram, new_gram)
            direction = residual + jnp.dot(dir_coef.T, direction, precision=HIGH)
        gram = new_gram
    rel_norms = jnp.sqrt(jnp.diagonal(new_gram) / jnp.diagonal(first))
    return (solution, residual, rel_norms)


def solution(mesh):
    placed = (P(None, ("row", "col")), P("row"), P(None, "row"))
    return jax.shard_map(
        on_device,
        mesh=mesh,
        in_specs=placed,
        out_specs=(P(None, "row"), P(None, "row"), P()),
        check_vma=False,
    )
```

```python
import functools
import math

import jax
import jax.numpy as jnp
from jax import lax
from jax.experimental import pallas as pl
from jax.experimental.pallas import tpu as pltpu
from jax.sharding import PartitionSpec as P

ITERS = 2
HIGH = lax.Precision.HIGHEST
MESH = pl.DeviceIdType.MESH
F32 = jnp.float32
BF16 = jnp.bfloat16


def bdot(first, second, dims):
    return lax.dot_general(first, second, (dims, ((), ())), preferred_element_type=F32)


def fdot(first, second, dims):
    return lax.dot_general(
        first, second, (dims, ((), ())), precision=HIGH, preferred_element_type=F32
    )


NT = ((1,), (1,))
TN = ((0,), (0,))
NN = ((1,), (0,))


def split2(value):
    high = value.astype(BF16)
    return high, (value - high.astype(F32)).astype(BF16)


def split3(value):
    high = value.astype(BF16)
    rest = value - high.astype(F32)
    mid = rest.astype(BF16)
    return high, mid, (rest - mid.astype(F32)).astype(BF16)


def solve_panels(matrix, target, out):
    size = matrix.shape[0]
    matrix = 0.5 * (matrix + matrix.T)
    both = jnp.concatenate([target, matrix], axis=1)
    width = both.shape[1]
    base = target.shape[1]
    panels = size // 8
    tiles = [both[8 * t : 8 * t + 8] for t in range(panels)]
    sublane = lax.broadcasted_iota(jnp.int32, (8, width), 0)

    def lane(tile, j):
        return jnp.broadcast_to(tile[:, j : j + 1], (8, width))

    def row(tile, s):
        return jnp.broadcast_to(tile[s : s + 1, :], (8, width))

    for k in range(panels):
        start = base + 8 * k
        cols = [lane(tiles[k], start + j) for j in range(8)]
        others = {
            t: [lane(tiles[t], start + j) for j in range(8)]
            for t in range(panels)
            if t != k
        }
        panel = tiles[k]
        for s in range(8):
            scale = 1.0 / row(cols[s], s)
            here = sublane == s
            factor = cols[s]

            def step(value):
                pivot = row(value, s) * scale
                return jnp.where(here, pivot, value - factor * pivot)

            panel = step(panel)
            for j in range(s + 1, 8):
                cols[j] = step(cols[j])
        rows = [row(panel, s) for s in range(8)]
        tiles[k] = panel
        for t in others:
            total = others[t][0] * rows[0]
            for s in range(1, 8):
                total = total + others[t][s] * rows[s]
            tiles[t] = tiles[t] - total
        if k + 1 < panels:
            yield
    out.append(jnp.concatenate(tiles, axis=0)[:, :base])
    yield


def solve_spd(matrix, target):
    out = []
    for _ in solve_panels(matrix, target, out):
        pass
    return out[0]


def kernel_body(
    n_row, n_col,
    pts_ref, noise_ref, rhs_ref,
    sol_ref, res_ref, rel_ref,
    pbuf, rbuf, nbuf, left, right, khi, klo, rs, qs, ss, img, next_res, dirs,
    pzsem, pzsend, pcsem, pcsend, nsem, nsend, zsem, zsend, csem, csend,
):
    z = lax.axis_index("row")
    c = lax.axis_index("col")
    dim, piece = pts_ref.shape
    rhs_count, block = rhs_ref.shape
    total = block * n_row
    half_rows = rhs_count // 2
    core = lax.rem(c, 2)
    partner = (z, c + 1 - 2 * core)

    pbuf[c, z] = pts_ref[...]
    nbuf[z] = noise_ref[...]
    rbuf[z] = rhs_ref[...]
    barrier = pltpu.get_barrier_semaphore()
    for dz in range(1, n_row):
        pl.semaphore_signal(barrier, inc=1, device_id=(lax.rem(z + dz, n_row), c), device_id_type=MESH)
    for dc in range(1, n_col):
        pl.semaphore_signal(barrier, inc=1, device_id=(z, lax.rem(c + dc, n_col)), device_id_type=MESH)
    pl.semaphore_wait(barrier, n_row + n_col - 2)

    mine = pl.ds(pl.multiple_of(core * half_rows, half_rows), half_rows)
    copies = []

    def send(src, dst, ssem, rsem, device):
        copy = pltpu.make_async_remote_copy(
            src_ref=src, dst_ref=dst, send_sem=ssem, recv_sem=rsem,
            device_id=device, device_id_type=MESH,
        )
        copy.start()
        copies.append(copy)
        return copy

    p_z, r_z, n_z = [None], [None], [None]
    for dz in range(1, n_row):
        dev = (lax.rem(z + dz, n_row), c)
        p_z.append(send(pts_ref, pbuf.at[c, z], pzsend.at[dz], pzsem.at[dz], dev))
    for dz in range(1, n_row):
        dev = (lax.rem(z + dz, n_row), c)
        r_z.append(send(rhs_ref.at[mine, :], rbuf.at[z, mine, :], zsend.at[dz], zsem.at[dz], dev))
    for dz in range(1, n_row):
        dev = (lax.rem(z + dz, n_row), c)
        n_z.append(send(noise_ref, nbuf.at[z], nsend.at[dz], nsem.at[dz], dev))
    for dz in range(1, n_row):
        p_z[dz].wait_recv()
    p_c = [None]
    for dc in range(1, n_col):
        dev = (z, lax.rem(c + dc, n_col))
        p_c.append(send(pbuf.at[c], pbuf.at[c], pcsend.at[dc], pcsem.at[dc], dev))
    for dc in range(1, n_col):
        p_c[dc].wait_recv()

    pair = 128 // piece
    for zz in range(n_row):
        for m in range(n_col // pair):
            x = jnp.concatenate([pbuf[m * pair + q, zz] for q in range(pair)], axis=1)
            half = -0.5 * jnp.sum(x * x, axis=0, keepdims=True)
            one = jnp.ones_like(half)
            pad = jnp.zeros((16 - dim - 2, pair * piece), F32)
            lh, lm, ll = split3(jnp.concatenate([x, half, one, pad], axis=0))
            rh, rm, rl = split3(jnp.concatenate([x, one, half, pad], axis=0))
            at = pl.ds(zz * block + m * pair * piece, pair * piece)
            left[:, at] = jnp.concatenate([lh, lh, lm, lh, ll, lm], axis=0)
            right[:, at] = jnp.concatenate([rh, rm, rh, rl, rh, rm], axis=0)

    tile = 256
    wide = 512

    def build(t, carry):
        at = pl.ds(pl.multiple_of(t * tile, tile), tile)
        lhs = left[:, at]
        for w in range(total // wide):
            cols = pl.ds(w * wide, wide)
            high, low = split2(jnp.exp(bdot(lhs, right[:, cols], TN)))
            khi[at, cols] = high
            klo[at, cols] = low
        return carry

    tiles = total // tile
    steps = [tiles * (q + 1) // n_row for q in range(n_row)]
    r_c = [None]
    done = 0
    for dz in range(1, n_row):
        lax.fori_loop(done, steps[dz - 1], build, 0)
        done = steps[dz - 1]
        src_z = lax.rem(z + n_row - dz, n_row)
        r_z[dz].wait_recv()
        part = rbuf.at[src_z, mine, :]
        r_c.append(send(part, part, csend.at[dz], csem.at[dz], partner))
    lax.fori_loop(done, tiles, build, 0)
    for dz in range(1, n_row):
        n_z[dz].wait_recv()
        r_c[dz].wait_recv()
    for copy in copies:
        copy.wait_send()

    top = pl.ds(0, rhs_count)
    low_half = pl.ds(rhs_count, rhs_count)

    def keep(stack, at, value):
        high, low = split2(value)
        stack[top, at] = high
        stack[low_half, at] = low

    def products(first, second):
        out = bdot(first[...], second[...], NT)
        upper, lower = out[:rhs_count], out[rhs_count:]
        both = upper + lower
        return both[:, :rhs_count] + both[:, rhs_count:]

    def weights(coef):
        turned = coef.T
        high, low = split2(jnp.concatenate([turned, turned], axis=1))
        return jnp.concatenate([high, low], axis=0)

    def apply(stacked, source):
        out = bdot(stacked, source, NN)
        return out[:rhs_count] + out[rhs_count:]

    chunk = min(256, block)
    spots = [
        (zz, pl.ds(q * chunk, chunk), pl.ds(zz * block + q * chunk, chunk))
        for zz in range(n_row)
        for q in range(block // chunk)
    ]

    def operate(source, stack, beside=None):
        for zz, inner, cols in spots:
            main = bdot(stack[...], khi[:, cols], NN)
            minor = bdot(stack[top, :], klo[:, cols], NN)
            value = (main[:rhs_count] + (main[rhs_count:] + minor)) + nbuf[zz, :, inner] * source[zz, :, inner]
            img[zz, :, inner] = value
            keep(qs, cols, value)
            if beside is not None:
                next(beside, None)

    def square_sums(squares):
        return fdot(jnp.ones((8, squares.shape[1]), F32), squares, NT)

    own = pl.ds(pl.multiple_of(z * block, block), block)
    first_squares = jnp.zeros((rhs_count, chunk), F32)
    for zz, inner, cols in spots:
        base = rbuf[zz, :, inner]
        keep(rs, cols, base)
        first_squares = first_squares + base * base
    gram = products(rs, rs)
    same = lax.broadcasted_iota(jnp.int32, gram.shape, 0) == lax.broadcasted_iota(jnp.int32, gram.shape, 1)
    inverse = []
    beside = solve_panels(gram, same.astype(F32), inverse)
    operate(rbuf, rs, beside)
    for _ in beside:
        pass
    first_sum = square_sums(first_squares)
    stacked = weights(solve_spd(products(rs, qs), gram))
    for zz, inner, cols in spots:
        value = rbuf[zz, :, inner] - apply(stacked, qs[:, cols])
        next_res[zz, :, inner] = value
        keep(ss, cols, value)
    my_sol = apply(stacked, rs[:, own])
    gram = products(ss, ss)
    stacked = weights(fdot(inverse[0], gram, NN))
    for zz, inner, cols in spots:
        value = next_res[zz, :, inner] + apply(stacked, rs[:, cols])
        dirs[zz, :, inner] = value
        keep(ss, cols, value)
    operate(dirs, ss)
    stacked = weights(solve_spd(products(ss, qs), gram))
    last_squares = jnp.zeros((rhs_count, chunk), F32)
    for zz, inner, cols in spots:
        value = next_res[zz, :, inner] - apply(stacked, qs[:, cols])
        last_squares = last_squares + value * value
    sol_ref[...] = my_sol + apply(stacked, ss[:, own])
    res_ref[...] = next_res[z] - apply(stacked, qs[:, own])
    rel_ref[...] = jnp.sqrt(square_sums(last_squares) / first_sum)[0:1]


def fits(n_row, n_col, points, right_sides):
    rhs_count, block = right_sides.shape
    dim, piece = points.shape
    total = block * n_row
    return (
        rhs_count == 64
        and n_col % 2 == 0
        and 128 % piece == 0
        and n_col % (128 // piece) == 0
        and total % 512 == 0
        and block % 128 == 0
        and dim <= 14
        and total * total * 4 <= 20 * 2**20
    )


def fused(points, noise_level, right_sides):
    n_row = lax.axis_size("row")
    n_col = lax.axis_size("col")
    rhs_count, block = right_sides.shape
    dim, piece = points.shape
    total = block * n_row
    vmem = pl.BlockSpec(memory_space=pltpu.VMEM)
    sol, res, rel = pl.pallas_call(
        functools.partial(kernel_body, n_row, n_col),
        out_shape=(
            jax.ShapeDtypeStruct((rhs_count, block), F32),
            jax.ShapeDtypeStruct((rhs_count, block), F32),
            jax.ShapeDtypeStruct((1, rhs_count), F32),
        ),
        in_specs=[vmem] * 3,
        out_specs=(vmem,) * 3,
        scratch_shapes=[
            pltpu.VMEM((n_col, n_row, dim, piece), F32),
            pltpu.VMEM((n_row, rhs_count, block), F32),
            pltpu.VMEM((n_row, 1, block), F32),
            pltpu.VMEM((96, total), BF16),
            pltpu.VMEM((96, total), BF16),
            pltpu.VMEM((total, total), BF16),
            pltpu.VMEM((total, total), BF16),
            pltpu.VMEM((2 * rhs_count, total), BF16),
            pltpu.VMEM((2 * rhs_count, total), BF16),
            pltpu.VMEM((2 * rhs_count, total), BF16),
            pltpu.VMEM((n_row, rhs_count, block), F32),
            pltpu.VMEM((n_row, rhs_count, block), F32),
            pltpu.VMEM((n_row, rhs_count, block), F32),
            pltpu.SemaphoreType.DMA((n_row,)),
            pltpu.SemaphoreType.DMA((n_row,)),
            pltpu.SemaphoreType.DMA((n_col,)),
            pltpu.SemaphoreType.DMA((n_col,)),
            pltpu.SemaphoreType.DMA((n_row,)),
            pltpu.SemaphoreType.DMA((n_row,)),
            pltpu.SemaphoreType.DMA((n_row,)),
            pltpu.SemaphoreType.DMA((n_row,)),
            pltpu.SemaphoreType.DMA((n_row,)),
            pltpu.SemaphoreType.DMA((n_row,)),
        ],
        compiler_params=pltpu.CompilerParams(
            collective_id=0, has_side_effects=True, vmem_limit_bytes=60 * 2**20
        ),
    )(points, noise_level[None, :], right_sides)
    return sol, res, rel[0]


def from_root(value, axis, root):
    mine = lax.axis_index(axis) == root
    return lax.psum(jnp.where(mine, value, jnp.zeros_like(value)), axis)


def products(first, second):
    return lax.dot_general(first, second, (((1,), (1,)), ((), ())), precision=HIGH)


def solve_sym(matrix, target):
    lower = jnp.linalg.cholesky(0.5 * (matrix + matrix.T))
    return jax.scipy.linalg.cho_solve((lower, True), target)


def gram_sum(single):
    return lax.psum(single, "row")


def triple_sum(first, second, third):
    return lax.psum((first, second, third), "row")


def on_device(points, noise_level, right_sides):
    row_count = lax.axis_size("row")
    col_count = lax.axis_size("col")
    if fits(row_count, col_count, points, right_sides):
        return fused(points, noise_level, right_sides)
    row_index = lax.axis_index("row")
    col_index = lax.axis_index("col")
    pts_dev = points.shape[1]
    row_len = pts_dev * col_count
    col_len = pts_dev * row_count
    col_ratio = col_count // row_count
    all_points = lax.all_gather(points, ("row", "col"), axis=1, tiled=True)
    sq_norms = jnp.sum(all_points * all_points, axis=0)
    row_points = lax.dynamic_slice_in_dim(all_points, row_index * row_len, row_len, 1)
    row_sq = lax.dynamic_slice_in_dim(sq_norms, row_index * row_len, row_len, 0)
    col_points = lax.dynamic_slice_in_dim(all_points, col_index * col_len, col_len, 1)
    col_sq = lax.dynamic_slice_in_dim(sq_norms, col_index * col_len, col_len, 0)
    tile_rows = math.gcd(row_len, 512)
    tile_count = row_len // tile_rows
    rhs_count = right_sides.shape[0]
    residual = right_sides
    solution = jnp.zeros_like(residual)
    direction = residual
    gram = gram_sum(products(residual, residual))
    first = gram
    new_gram = gram
    for iteration in range(ITERS):
        source = lax.dynamic_slice_in_dim(direction, col_index % col_ratio * col_len, col_len, 1)
        col_direction = from_root(source, "row", col_index // col_ratio)

        def one_tile(index, result):
            offset = index * tile_rows
            tile_points = lax.dynamic_slice_in_dim(row_points, offset, tile_rows, 1)
            tile_sq = lax.dynamic_slice_in_dim(row_sq, offset, tile_rows, 0)
            sq_dist = (
                tile_sq[:, None]
                + col_sq[None, :]
                - 2.0 * jnp.dot(tile_points.T, col_points, precision=HIGH)
            )
            kernel = jnp.exp(-0.5 * sq_dist)
            return lax.dynamic_update_slice_in_dim(
                result, products(col_direction, kernel), offset, 1
            )

        image = (
            lax.psum(
                lax.fori_loop(
                    0, tile_count, one_tile, jnp.zeros((rhs_count, row_len), jnp.float32)
                ),
                "col",
            )
            + noise_level[None, :] * direction
        )
        curv, cross, image_gram = triple_sum(
            products(direction, image), products(residual, image), products(image, image)
        )
        step_coef = solve_sym(curv, gram)
        solution = solution + jnp.dot(step_coef.T, direction, precision=HIGH)
        residual = residual - jnp.dot(step_coef.T, image, precision=HIGH)
        cross_coef = jnp.dot(cross, step_coef, precision=HIGH)
        quad = jnp.dot(step_coef.T, jnp.dot(image_gram, step_coef, precision=HIGH), precision=HIGH)
        new_gram = gram - cross_coef - cross_coef.T + quad
        if iteration + 1 < ITERS:
            dir_coef = solve_sym(gram, new_gram)
            direction = residual + jnp.dot(dir_coef.T, direction, precision=HIGH)
        gram = new_gram
    rel_norms = jnp.sqrt(jnp.diagonal(new_gram) / jnp.diagonal(first))
    return (solution, residual, rel_norms)


def solution(mesh):
    placed = (P(None, ("row", "col")), P("row"), P(None, "row"))
    return jax.shard_map(
        on_device,
        mesh=mesh,
        in_specs=placed,
        out_specs=(P(None, "row"), P(None, "row"), P()),
        check_vma=False,
    )
```

```python
import functools
import math

import jax
import jax.numpy as jnp
from jax import lax
from jax.experimental import pallas as pl
from jax.experimental.pallas import tpu as pltpu
from jax.sharding import PartitionSpec as P

ITERS = 2
HIGH = lax.Precision.HIGHEST
MESH = pl.DeviceIdType.MESH
F32 = jnp.float32
BF16 = jnp.bfloat16


def bdot(first, second, dims):
    return lax.dot_general(first, second, (dims, ((), ())), preferred_element_type=F32)


def fdot(first, second, dims):
    return lax.dot_general(
        first, second, (dims, ((), ())), precision=HIGH, preferred_element_type=F32
    )


NT = ((1,), (1,))
TN = ((0,), (0,))
NN = ((1,), (0,))


def split2(value):
    high = value.astype(BF16)
    return high, (value - high.astype(F32)).astype(BF16)


def split3(value):
    high = value.astype(BF16)
    rest = value - high.astype(F32)
    mid = rest.astype(BF16)
    return high, mid, (rest - mid.astype(F32)).astype(BF16)


def solve_start(matrix, target):
    matrix = 0.5 * (matrix + matrix.T)
    both = jnp.concatenate([matrix, target], axis=1)
    return tuple(both[8 * t : 8 * t + 8] for t in range(matrix.shape[0] // 8))


def solve_panel(tiles):
    width = tiles[0].shape[1]
    sublane = lax.broadcasted_iota(jnp.int32, (8, width), 0)

    def lane(tile, j):
        return jnp.broadcast_to(tile[:, j : j + 1], (8, width))

    def row(tile, s):
        return jnp.broadcast_to(tile[s : s + 1, :], (8, width))

    def turn(tile):
        return pltpu.roll(tile, width - 8, 1)

    cols = [lane(tiles[0], j) for j in range(8)]
    others = [[lane(tile, j) for j in range(8)] for tile in tiles[1:]]
    panel = turn(tiles[0])
    rest = [turn(tile) for tile in tiles[1:]]
    for s in range(8):
        scale = 1.0 / row(cols[s], s)
        here = sublane == s
        factor = cols[s]

        def step(value):
            pivot = row(value, s) * scale
            return jnp.where(here, pivot, value - factor * pivot)

        panel = step(panel)
        for j in range(s + 1, 8):
            cols[j] = step(cols[j])
    rows = [row(panel, s) for s in range(8)]
    out = []
    for tile, factors in zip(rest, others):
        total = factors[0] * rows[0]
        for s in range(1, 8):
            total = total + factors[s] * rows[s]
        out.append(tile - total)
    return tuple(out) + (panel,)


def solve_end(tiles):
    return jnp.concatenate(tiles, axis=0)[:, : 8 * len(tiles)]


def solve_spd(matrix, target):
    tiles = solve_start(matrix, target)
    return solve_end(lax.fori_loop(0, len(tiles), lambda _, now: solve_panel(now), tiles))


def kernel_body(
    n_row, n_col,
    pts_ref, noise_ref, rhs_ref,
    sol_ref, res_ref, rel_ref,
    pbuf, rbuf, nbuf, left, right, khi, klo, rs, qs, ss, img, next_res, dirs,
    pzsem, pzsend, pcsem, pcsend, nsem, nsend, zsem, zsend, csem, csend, lsem,
):
    z = lax.axis_index("row")
    c = lax.axis_index("col")
    dim, piece = pts_ref.shape
    rhs_count, block = rhs_ref.shape
    total = block * n_row
    half_rows = rhs_count // 2
    core = lax.rem(c, 2)
    partner = (z, c + 1 - 2 * core)

    local = [
        pltpu.make_async_copy(pts_ref, pbuf.at[c, z], lsem.at[0]),
        pltpu.make_async_copy(rhs_ref, rbuf.at[z], lsem.at[1]),
        pltpu.make_async_copy(noise_ref, nbuf.at[z], lsem.at[2]),
    ]
    for copy in local:
        copy.start()
    barrier = pltpu.get_barrier_semaphore()
    for dz in range(1, n_row):
        pl.semaphore_signal(barrier, inc=1, device_id=(lax.rem(z + dz, n_row), c), device_id_type=MESH)
    for dc in range(1, n_col):
        pl.semaphore_signal(barrier, inc=1, device_id=(z, lax.rem(c + dc, n_col)), device_id_type=MESH)
    pl.semaphore_wait(barrier, n_row + n_col - 2)
    for copy in local:
        copy.wait()

    mine = pl.ds(pl.multiple_of(core * half_rows, half_rows), half_rows)
    copies = []

    def send(src, dst, ssem, rsem, device):
        copy = pltpu.make_async_remote_copy(
            src_ref=src, dst_ref=dst, send_sem=ssem, recv_sem=rsem,
            device_id=device, device_id_type=MESH,
        )
        copy.start()
        copies.append(copy)
        return copy

    p_z, r_z, n_z = [None], [None], [None]
    for dz in range(1, n_row):
        dev = (lax.rem(z + dz, n_row), c)
        p_z.append(send(pbuf.at[c, z], pbuf.at[c, z], pzsend.at[dz], pzsem.at[dz], dev))
    for dz in range(1, n_row):
        dev = (lax.rem(z + dz, n_row), c)
        r_z.append(send(rbuf.at[z, mine, :], rbuf.at[z, mine, :], zsend.at[dz], zsem.at[dz], dev))
    for dz in range(1, n_row):
        dev = (lax.rem(z + dz, n_row), c)
        n_z.append(send(nbuf.at[z], nbuf.at[z], nsend.at[dz], nsem.at[dz], dev))
    for dz in range(1, n_row):
        p_z[dz].wait_recv()
    p_c = [None]
    for dc in range(1, n_col):
        dev = (z, lax.rem(c + dc, n_col))
        p_c.append(send(pbuf.at[c], pbuf.at[c], pcsend.at[dc], pcsem.at[dc], dev))
    for dc in range(1, n_col):
        p_c[dc].wait_recv()

    pair = 128 // piece
    for zz in range(n_row):
        for m in range(n_col // pair):
            x = jnp.concatenate([pbuf[m * pair + q, zz] for q in range(pair)], axis=1)
            half = -0.5 * jnp.sum(x * x, axis=0, keepdims=True)
            one = jnp.ones_like(half)
            pad = jnp.zeros((16 - dim - 2, pair * piece), F32)
            lh, lm, ll = split3(jnp.concatenate([x, half, one, pad], axis=0))
            rh, rm, rl = split3(jnp.concatenate([x, one, half, pad], axis=0))
            at = pl.ds(zz * block + m * pair * piece, pair * piece)
            left[:, at] = jnp.concatenate([lh, lh, lm, lh, ll, lm], axis=0)
            right[:, at] = jnp.concatenate([rh, rm, rh, rl, rh, rm], axis=0)

    tile = 256
    wide = 512

    def build(t, carry):
        at = pl.ds(pl.multiple_of(t * tile, tile), tile)
        lhs = left[:, at]
        for w in range(total // wide):
            cols = pl.ds(w * wide, wide)
            high, low = split2(jnp.exp(bdot(lhs, right[:, cols], TN)))
            khi[at, cols] = high
            klo[at, cols] = low
        return carry

    tiles = total // tile
    steps = [tiles * (q + 1) // n_row for q in range(n_row)]
    r_c = [None]
    done = 0
    for dz in range(1, n_row):
        lax.fori_loop(done, steps[dz - 1], build, 0)
        done = steps[dz - 1]
        src_z = lax.rem(z + n_row - dz, n_row)
        r_z[dz].wait_recv()
        part = rbuf.at[src_z, mine, :]
        r_c.append(send(part, part, csend.at[dz], csem.at[dz], partner))
    lax.fori_loop(done, tiles, build, 0)
    for dz in range(1, n_row):
        n_z[dz].wait_recv()
        r_c[dz].wait_recv()
    for copy in copies:
        copy.wait_send()

    top = pl.ds(0, rhs_count)
    low_half = pl.ds(rhs_count, rhs_count)

    def keep(stack, at, value):
        high, low = split2(value)
        stack[top, at] = high
        stack[low_half, at] = low

    def products(first, second):
        out = bdot(first[...], second[...], NT)
        upper, lower = out[:rhs_count], out[rhs_count:]
        both = upper + lower
        return both[:, :rhs_count] + both[:, rhs_count:]

    def weights(coef):
        turned = coef.T
        high, low = split2(jnp.concatenate([turned, turned], axis=1))
        return jnp.concatenate([high, low], axis=0)

    def apply(stacked, source):
        out = bdot(stacked, source, NN)
        return out[:rhs_count] + out[rhs_count:]

    chunk = min(256, block)
    spots = [
        (zz, pl.ds(q * chunk, chunk), pl.ds(zz * block + q * chunk, chunk))
        for zz in range(n_row)
        for q in range(block // chunk)
    ]

    panels = rhs_count // 8

    def operate(source, stack, tiles=()):
        per = panels // n_row if panels % n_row == 0 else panels

        def one_block(zz, tiles):
            cols = pl.ds(pl.multiple_of(zz * block, block), block)
            main = bdot(stack[...], khi[:, cols], NN)
            minor = bdot(stack[top, :], klo[:, cols], NN)
            if tiles and per < panels:
                for _ in range(per):
                    tiles = solve_panel(tiles)
            value = (main[:rhs_count] + (main[rhs_count:] + minor)) + nbuf[zz] * source[zz]
            img[zz] = value
            keep(qs, cols, value)
            return tiles

        tiles = lax.fori_loop(0, n_row, one_block, tiles)
        if tiles and per == panels:
            for _ in range(panels):
                tiles = solve_panel(tiles)
        return tiles

    def square_sums(squares):
        return fdot(jnp.ones((8, squares.shape[1]), F32), squares, NT)

    own = pl.ds(pl.multiple_of(z * block, block), block)
    first_squares = jnp.zeros((rhs_count, chunk), F32)
    for zz, inner, cols in spots:
        base = rbuf[zz, :, inner]
        keep(rs, cols, base)
        first_squares = first_squares + base * base
    gram = products(rs, rs)
    same = lax.broadcasted_iota(jnp.int32, gram.shape, 0) == lax.broadcasted_iota(jnp.int32, gram.shape, 1)
    inverse = solve_end(operate(rbuf, rs, solve_start(gram, same.astype(F32))))
    first_sum = square_sums(first_squares)
    stacked = weights(solve_spd(products(rs, qs), gram))
    for zz, inner, cols in spots:
        value = rbuf[zz, :, inner] - apply(stacked, qs[:, cols])
        next_res[zz, :, inner] = value
        keep(ss, cols, value)
    my_sol = apply(stacked, rs[:, own])
    gram = products(ss, ss)
    stacked = weights(fdot(inverse, gram, NN))
    for zz, inner, cols in spots:
        value = next_res[zz, :, inner] + apply(stacked, rs[:, cols])
        dirs[zz, :, inner] = value
        keep(ss, cols, value)
    operate(dirs, ss)
    stacked = weights(solve_spd(products(ss, qs), gram))
    last_squares = jnp.zeros((rhs_count, chunk), F32)
    for zz, inner, cols in spots:
        value = next_res[zz, :, inner] - apply(stacked, qs[:, cols])
        last_squares = last_squares + value * value
    sol_ref[...] = my_sol + apply(stacked, ss[:, own])
    res_ref[...] = next_res[z] - apply(stacked, qs[:, own])
    rel_ref[...] = jnp.sqrt(square_sums(last_squares) / first_sum)[0:1]


def fits(n_row, n_col, points, right_sides):
    rhs_count, block = right_sides.shape
    dim, piece = points.shape
    total = block * n_row
    return (
        rhs_count == 64
        and n_col % 2 == 0
        and 128 % piece == 0
        and n_col % (128 // piece) == 0
        and total % 512 == 0
        and block % 128 == 0
        and dim <= 14
        and total * total * 4 <= 20 * 2**20
    )


def fused(points, noise_level, right_sides):
    n_row = lax.axis_size("row")
    n_col = lax.axis_size("col")
    rhs_count, block = right_sides.shape
    dim, piece = points.shape
    total = block * n_row
    vmem = pl.BlockSpec(memory_space=pltpu.VMEM)
    sol, res, rel = pl.pallas_call(
        functools.partial(kernel_body, n_row, n_col),
        out_shape=(
            jax.ShapeDtypeStruct((rhs_count, block), F32),
            jax.ShapeDtypeStruct((rhs_count, block), F32),
            jax.ShapeDtypeStruct((1, rhs_count), F32),
        ),
        in_specs=[pl.BlockSpec(memory_space=pl.ANY)] * 3,
        out_specs=(vmem,) * 3,
        scratch_shapes=[
            pltpu.VMEM((n_col, n_row, dim, piece), F32),
            pltpu.VMEM((n_row, rhs_count, block), F32),
            pltpu.VMEM((n_row, 1, block), F32),
            pltpu.VMEM((96, total), BF16),
            pltpu.VMEM((96, total), BF16),
            pltpu.VMEM((total, total), BF16),
            pltpu.VMEM((total, total), BF16),
            pltpu.VMEM((2 * rhs_count, total), BF16),
            pltpu.VMEM((2 * rhs_count, total), BF16),
            pltpu.VMEM((2 * rhs_count, total), BF16),
            pltpu.VMEM((n_row, rhs_count, block), F32),
            pltpu.VMEM((n_row, rhs_count, block), F32),
            pltpu.VMEM((n_row, rhs_count, block), F32),
            pltpu.SemaphoreType.DMA((n_row,)),
            pltpu.SemaphoreType.DMA((n_row,)),
            pltpu.SemaphoreType.DMA((n_col,)),
            pltpu.SemaphoreType.DMA((n_col,)),
            pltpu.SemaphoreType.DMA((n_row,)),
            pltpu.SemaphoreType.DMA((n_row,)),
            pltpu.SemaphoreType.DMA((n_row,)),
            pltpu.SemaphoreType.DMA((n_row,)),
            pltpu.SemaphoreType.DMA((n_row,)),
            pltpu.SemaphoreType.DMA((n_row,)),
            pltpu.SemaphoreType.DMA((3,)),
        ],
        compiler_params=pltpu.CompilerParams(
            collective_id=0, has_side_effects=True, vmem_limit_bytes=60 * 2**20
        ),
    )(points, noise_level[None, :], right_sides)
    return sol, res, rel[0]


def from_root(value, axis, root):
    mine = lax.axis_index(axis) == root
    return lax.psum(jnp.where(mine, value, jnp.zeros_like(value)), axis)


def products(first, second):
    return lax.dot_general(first, second, (((1,), (1,)), ((), ())), precision=HIGH)


def solve_sym(matrix, target):
    lower = jnp.linalg.cholesky(0.5 * (matrix + matrix.T))
    return jax.scipy.linalg.cho_solve((lower, True), target)


def gram_sum(single):
    return lax.psum(single, "row")


def triple_sum(first, second, third):
    return lax.psum((first, second, third), "row")


def on_device(points, noise_level, right_sides):
    row_count = lax.axis_size("row")
    col_count = lax.axis_size("col")
    if fits(row_count, col_count, points, right_sides):
        return fused(points, noise_level, right_sides)
    row_index = lax.axis_index("row")
    col_index = lax.axis_index("col")
    pts_dev = points.shape[1]
    row_len = pts_dev * col_count
    col_len = pts_dev * row_count
    col_ratio = col_count // row_count
    all_points = lax.all_gather(points, ("row", "col"), axis=1, tiled=True)
    sq_norms = jnp.sum(all_points * all_points, axis=0)
    row_points = lax.dynamic_slice_in_dim(all_points, row_index * row_len, row_len, 1)
    row_sq = lax.dynamic_slice_in_dim(sq_norms, row_index * row_len, row_len, 0)
    col_points = lax.dynamic_slice_in_dim(all_points, col_index * col_len, col_len, 1)
    col_sq = lax.dynamic_slice_in_dim(sq_norms, col_index * col_len, col_len, 0)
    tile_rows = math.gcd(row_len, 512)
    tile_count = row_len // tile_rows
    rhs_count = right_sides.shape[0]
    residual = right_sides
    solution = jnp.zeros_like(residual)
    direction = residual
    gram = gram_sum(products(residual, residual))
    first = gram
    new_gram = gram
    for iteration in range(ITERS):
        source = lax.dynamic_slice_in_dim(direction, col_index % col_ratio * col_len, col_len, 1)
        col_direction = from_root(source, "row", col_index // col_ratio)

        def one_tile(index, result):
            offset = index * tile_rows
            tile_points = lax.dynamic_slice_in_dim(row_points, offset, tile_rows, 1)
            tile_sq = lax.dynamic_slice_in_dim(row_sq, offset, tile_rows, 0)
            sq_dist = (
                tile_sq[:, None]
                + col_sq[None, :]
                - 2.0 * jnp.dot(tile_points.T, col_points, precision=HIGH)
            )
            kernel = jnp.exp(-0.5 * sq_dist)
            return lax.dynamic_update_slice_in_dim(
                result, products(col_direction, kernel), offset, 1
            )

        image = (
            lax.psum(
                lax.fori_loop(
                    0, tile_count, one_tile, jnp.zeros((rhs_count, row_len), jnp.float32)
                ),
                "col",
            )
            + noise_level[None, :] * direction
        )
        curv, cross, image_gram = triple_sum(
            products(direction, image), products(residual, image), products(image, image)
        )
        step_coef = solve_sym(curv, gram)
        solution = solution + jnp.dot(step_coef.T, direction, precision=HIGH)
        residual = residual - jnp.dot(step_coef.T, image, precision=HIGH)
        cross_coef = jnp.dot(cross, step_coef, precision=HIGH)
        quad = jnp.dot(step_coef.T, jnp.dot(image_gram, step_coef, precision=HIGH), precision=HIGH)
        new_gram = gram - cross_coef - cross_coef.T + quad
        if iteration + 1 < ITERS:
            dir_coef = solve_sym(gram, new_gram)
            direction = residual + jnp.dot(dir_coef.T, direction, precision=HIGH)
        gram = new_gram
    rel_norms = jnp.sqrt(jnp.diagonal(new_gram) / jnp.diagonal(first))
    return (solution, residual, rel_norms)


def solution(mesh):
    placed = (P(None, ("row", "col")), P("row"), P(None, "row"))
    return jax.shard_map(
        on_device,
        mesh=mesh,
        in_specs=placed,
        out_specs=(P(None, "row"), P(None, "row"), P()),
        check_vma=False,
    )
```

```python
import functools
import math

import jax
import jax.numpy as jnp
from jax import lax
from jax.experimental import pallas as pl
from jax.experimental.pallas import tpu as pltpu
from jax.sharding import PartitionSpec as P

ITERS = 2
HIGH = lax.Precision.HIGHEST
MESH = pl.DeviceIdType.MESH
F32 = jnp.float32
BF16 = jnp.bfloat16


def bdot(first, second, dims):
    return lax.dot_general(first, second, (dims, ((), ())), preferred_element_type=F32)


def fdot(first, second, dims):
    return lax.dot_general(
        first, second, (dims, ((), ())), precision=HIGH, preferred_element_type=F32
    )


NT = ((1,), (1,))
TN = ((0,), (0,))
NN = ((1,), (0,))


def split2(value):
    high = value.astype(BF16)
    return high, (value - high.astype(F32)).astype(BF16)


def split3(value):
    high = value.astype(BF16)
    rest = value - high.astype(F32)
    mid = rest.astype(BF16)
    return high, mid, (rest - mid.astype(F32)).astype(BF16)


def solve_start(matrix, target):
    matrix = 0.5 * (matrix + matrix.T)
    both = jnp.concatenate([matrix, target], axis=1)
    return tuple(both[8 * t : 8 * t + 8] for t in range(matrix.shape[0] // 8))


def solve_panel(tiles):
    width = tiles[0].shape[1]
    sublane = lax.broadcasted_iota(jnp.int32, (8, width), 0)

    def lane(tile, j):
        return jnp.broadcast_to(tile[:, j : j + 1], (8, width))

    def row(tile, s):
        return jnp.broadcast_to(tile[s : s + 1, :], (8, width))

    def turn(tile):
        return pltpu.roll(tile, width - 8, 1)

    cols = [lane(tiles[0], j) for j in range(8)]
    others = [[lane(tile, j) for j in range(8)] for tile in tiles[1:]]
    panel = turn(tiles[0])
    rest = [turn(tile) for tile in tiles[1:]]
    for s in range(8):
        scale = 1.0 / row(cols[s], s)
        here = sublane == s
        factor = cols[s]

        def step(value):
            pivot = row(value, s) * scale
            return jnp.where(here, pivot, value - factor * pivot)

        panel = step(panel)
        for j in range(s + 1, 8):
            cols[j] = step(cols[j])
    rows = [row(panel, s) for s in range(8)]
    out = []
    for tile, factors in zip(rest, others):
        total = factors[0] * rows[0]
        for s in range(1, 8):
            total = total + factors[s] * rows[s]
        out.append(tile - total)
    return tuple(out) + (panel,)


def solve_end(tiles):
    return jnp.concatenate(tiles, axis=0)[:, : 8 * len(tiles)]


def solve_spd(matrix, target):
    tiles = solve_start(matrix, target)
    return solve_end(lax.fori_loop(0, len(tiles), lambda _, now: solve_panel(now), tiles))


def kernel_body(
    n_row, n_col,
    pts_ref, noise_ref, rhs_ref,
    sol_ref, res_ref, rel_ref,
    pbuf, rbuf, nbuf, left, right, khi, klo, rs, qs, ss, img, next_res, dirs,
    pzsem, pzsend, pcsem, pcsend, nsem, nsend, zsem, zsend, csem, csend, lsem,
):
    z = lax.axis_index("row")
    c = lax.axis_index("col")
    dim, piece = pts_ref.shape
    rhs_count, block = rhs_ref.shape
    total = block * n_row
    half_rows = rhs_count // 2
    core = lax.rem(c, 2)
    partner = (z, c + 1 - 2 * core)

    local = [
        pltpu.make_async_copy(pts_ref, pbuf.at[c, z], lsem.at[0]),
        pltpu.make_async_copy(rhs_ref, rbuf.at[z], lsem.at[1]),
        pltpu.make_async_copy(noise_ref, nbuf.at[z], lsem.at[2]),
    ]
    for copy in local:
        copy.start()
    barrier = pltpu.get_barrier_semaphore()
    for dz in range(1, n_row):
        pl.semaphore_signal(barrier, inc=1, device_id=(lax.rem(z + dz, n_row), c), device_id_type=MESH)
    for dc in range(1, n_col):
        pl.semaphore_signal(barrier, inc=1, device_id=(z, lax.rem(c + dc, n_col)), device_id_type=MESH)
    pl.semaphore_wait(barrier, n_row + n_col - 2)
    for copy in local:
        copy.wait()

    mine = pl.ds(pl.multiple_of(core * half_rows, half_rows), half_rows)
    copies = []

    def send(src, dst, ssem, rsem, device):
        copy = pltpu.make_async_remote_copy(
            src_ref=src, dst_ref=dst, send_sem=ssem, recv_sem=rsem,
            device_id=device, device_id_type=MESH,
        )
        copy.start()
        copies.append(copy)
        return copy

    p_z, r_z, n_z = [None], [None], [None]
    for dz in range(1, n_row):
        dev = (lax.rem(z + dz, n_row), c)
        p_z.append(send(pbuf.at[c, z], pbuf.at[c, z], pzsend.at[dz], pzsem.at[dz], dev))
    for dz in range(1, n_row):
        dev = (lax.rem(z + dz, n_row), c)
        r_z.append(send(rbuf.at[z, mine, :], rbuf.at[z, mine, :], zsend.at[dz], zsem.at[dz], dev))
    for dz in range(1, n_row):
        dev = (lax.rem(z + dz, n_row), c)
        n_z.append(send(nbuf.at[z], nbuf.at[z], nsend.at[dz], nsem.at[dz], dev))
    p_c = []
    for dz in range(n_row):
        if dz > 0:
            p_z[dz].wait_recv()
        from_z = lax.rem(z + n_row - dz, n_row)
        for dc in range(1, n_col):
            dev = (z, lax.rem(c + dc, n_col))
            p_c.append(send(pbuf.at[c, from_z], pbuf.at[c, from_z], pcsend.at[dz, dc], pcsem.at[dz, dc], dev))
    for copy in p_c:
        copy.wait_recv()

    pair = 128 // piece
    for zz in range(n_row):
        for m in range(n_col // pair):
            x = jnp.concatenate([pbuf[m * pair + q, zz] for q in range(pair)], axis=1)
            half = -0.5 * jnp.sum(x * x, axis=0, keepdims=True)
            one = jnp.ones_like(half)
            pad = jnp.zeros((16 - dim - 2, pair * piece), F32)
            lh, lm, ll = split3(jnp.concatenate([x, half, one, pad], axis=0))
            rh, rm, rl = split3(jnp.concatenate([x, one, half, pad], axis=0))
            at = pl.ds(zz * block + m * pair * piece, pair * piece)
            left[:, at] = jnp.concatenate([lh, lh, lm, lh, ll, lm], axis=0)
            right[:, at] = jnp.concatenate([rh, rm, rh, rl, rh, rm], axis=0)

    tile = 256
    wide = 512

    def build(t, carry):
        at = pl.ds(pl.multiple_of(t * tile, tile), tile)
        lhs = left[:, at]
        for w in range(total // wide):
            cols = pl.ds(w * wide, wide)
            high, low = split2(jnp.exp(bdot(lhs, right[:, cols], TN)))
            khi[at, cols] = high
            klo[at, cols] = low
        return carry

    tiles = total // tile
    steps = [tiles * (q + 1) // n_row for q in range(n_row)]
    r_c = [None]
    done = 0
    for dz in range(1, n_row):
        lax.fori_loop(done, steps[dz - 1], build, 0)
        done = steps[dz - 1]
        src_z = lax.rem(z + n_row - dz, n_row)
        r_z[dz].wait_recv()
        part = rbuf.at[src_z, mine, :]
        r_c.append(send(part, part, csend.at[dz], csem.at[dz], partner))
    lax.fori_loop(done, tiles, build, 0)
    for dz in range(1, n_row):
        n_z[dz].wait_recv()
        r_c[dz].wait_recv()
    for copy in copies:
        copy.wait_send()

    top = pl.ds(0, rhs_count)
    low_half = pl.ds(rhs_count, rhs_count)

    def keep(stack, at, value):
        high, low = split2(value)
        stack[top, at] = high
        stack[low_half, at] = low

    def products(first, second):
        out = bdot(first[...], second[...], NT)
        upper, lower = out[:rhs_count], out[rhs_count:]
        both = upper + lower
        return both[:, :rhs_count] + both[:, rhs_count:]

    def weights(coef):
        turned = coef.T
        high, low = split2(jnp.concatenate([turned, turned], axis=1))
        return jnp.concatenate([high, low], axis=0)

    def apply(stacked, source):
        out = bdot(stacked, source, NN)
        return out[:rhs_count] + out[rhs_count:]

    chunk = min(256, block)
    spots = [
        (zz, pl.ds(q * chunk, chunk), pl.ds(zz * block + q * chunk, chunk))
        for zz in range(n_row)
        for q in range(block // chunk)
    ]

    panels = rhs_count // 8

    def operate(source, stack, tiles=()):
        per = panels // n_row if panels % n_row == 0 else panels

        def one_block(zz, tiles):
            cols = pl.ds(pl.multiple_of(zz * block, block), block)
            main = bdot(stack[...], khi[:, cols], NN)
            minor = bdot(stack[top, :], klo[:, cols], NN)
            if tiles and per < panels:
                for _ in range(per):
                    tiles = solve_panel(tiles)
            value = (main[:rhs_count] + (main[rhs_count:] + minor)) + nbuf[zz] * source[zz]
            img[zz] = value
            keep(qs, cols, value)
            return tiles

        tiles = lax.fori_loop(0, n_row, one_block, tiles)
        if tiles and per == panels:
            for _ in range(panels):
                tiles = solve_panel(tiles)
        return tiles

    def square_sums(squares):
        return fdot(jnp.ones((8, squares.shape[1]), F32), squares, NT)

    own = pl.ds(pl.multiple_of(z * block, block), block)
    first_squares = jnp.zeros((rhs_count, chunk), F32)
    for zz, inner, cols in spots:
        base = rbuf[zz, :, inner]
        keep(rs, cols, base)
        first_squares = first_squares + base * base
    gram = products(rs, rs)
    same = lax.broadcasted_iota(jnp.int32, gram.shape, 0) == lax.broadcasted_iota(jnp.int32, gram.shape, 1)
    inverse = solve_end(operate(rbuf, rs, solve_start(gram, same.astype(F32))))
    first_sum = square_sums(first_squares)
    stacked = weights(solve_spd(products(rs, qs), gram))
    for zz, inner, cols in spots:
        value = rbuf[zz, :, inner] - apply(stacked, qs[:, cols])
        next_res[zz, :, inner] = value
        keep(ss, cols, value)
    my_sol = apply(stacked, rs[:, own])
    gram = products(ss, ss)
    stacked = weights(fdot(inverse, gram, NN))
    for zz, inner, cols in spots:
        value = next_res[zz, :, inner] + apply(stacked, rs[:, cols])
        dirs[zz, :, inner] = value
        keep(ss, cols, value)
    operate(dirs, ss)
    stacked = weights(solve_spd(products(ss, qs), gram))
    last_squares = jnp.zeros((rhs_count, chunk), F32)
    for zz, inner, cols in spots:
        value = next_res[zz, :, inner] - apply(stacked, qs[:, cols])
        last_squares = last_squares + value * value
    sol_ref[...] = my_sol + apply(stacked, ss[:, own])
    res_ref[...] = next_res[z] - apply(stacked, qs[:, own])
    rel_ref[...] = jnp.sqrt(square_sums(last_squares) / first_sum)[0:1]


def fits(n_row, n_col, points, right_sides):
    rhs_count, block = right_sides.shape
    dim, piece = points.shape
    total = block * n_row
    return (
        rhs_count == 64
        and n_col % 2 == 0
        and 128 % piece == 0
        and n_col % (128 // piece) == 0
        and total % 512 == 0
        and block % 128 == 0
        and dim <= 14
        and total * total * 4 <= 20 * 2**20
    )


def fused(points, noise_level, right_sides):
    n_row = lax.axis_size("row")
    n_col = lax.axis_size("col")
    rhs_count, block = right_sides.shape
    dim, piece = points.shape
    total = block * n_row
    vmem = pl.BlockSpec(memory_space=pltpu.VMEM)
    sol, res, rel = pl.pallas_call(
        functools.partial(kernel_body, n_row, n_col),
        out_shape=(
            jax.ShapeDtypeStruct((rhs_count, block), F32),
            jax.ShapeDtypeStruct((rhs_count, block), F32),
            jax.ShapeDtypeStruct((1, rhs_count), F32),
        ),
        in_specs=[pl.BlockSpec(memory_space=pl.ANY)] * 3,
        out_specs=(vmem,) * 3,
        scratch_shapes=[
            pltpu.VMEM((n_col, n_row, dim, piece), F32),
            pltpu.VMEM((n_row, rhs_count, block), F32),
            pltpu.VMEM((n_row, 1, block), F32),
            pltpu.VMEM((96, total), BF16),
            pltpu.VMEM((96, total), BF16),
            pltpu.VMEM((total, total), BF16),
            pltpu.VMEM((total, total), BF16),
            pltpu.VMEM((2 * rhs_count, total), BF16),
            pltpu.VMEM((2 * rhs_count, total), BF16),
            pltpu.VMEM((2 * rhs_count, total), BF16),
            pltpu.VMEM((n_row, rhs_count, block), F32),
            pltpu.VMEM((n_row, rhs_count, block), F32),
            pltpu.VMEM((n_row, rhs_count, block), F32),
            pltpu.SemaphoreType.DMA((n_row,)),
            pltpu.SemaphoreType.DMA((n_row,)),
            pltpu.SemaphoreType.DMA((n_row, n_col)),
            pltpu.SemaphoreType.DMA((n_row, n_col)),
            pltpu.SemaphoreType.DMA((n_row,)),
            pltpu.SemaphoreType.DMA((n_row,)),
            pltpu.SemaphoreType.DMA((n_row,)),
            pltpu.SemaphoreType.DMA((n_row,)),
            pltpu.SemaphoreType.DMA((n_row,)),
            pltpu.SemaphoreType.DMA((n_row,)),
            pltpu.SemaphoreType.DMA((3,)),
        ],
        compiler_params=pltpu.CompilerParams(
            collective_id=0, has_side_effects=True, vmem_limit_bytes=60 * 2**20
        ),
    )(points, noise_level[None, :], right_sides)
    return sol, res, rel[0]


def from_root(value, axis, root):
    mine = lax.axis_index(axis) == root
    return lax.psum(jnp.where(mine, value, jnp.zeros_like(value)), axis)


def products(first, second):
    return lax.dot_general(first, second, (((1,), (1,)), ((), ())), precision=HIGH)


def solve_sym(matrix, target):
    lower = jnp.linalg.cholesky(0.5 * (matrix + matrix.T))
    return jax.scipy.linalg.cho_solve((lower, True), target)


def gram_sum(single):
    return lax.psum(single, "row")


def triple_sum(first, second, third):
    return lax.psum((first, second, third), "row")


def on_device(points, noise_level, right_sides):
    row_count = lax.axis_size("row")
    col_count = lax.axis_size("col")
    if fits(row_count, col_count, points, right_sides):
        return fused(points, noise_level, right_sides)
    row_index = lax.axis_index("row")
    col_index = lax.axis_index("col")
    pts_dev = points.shape[1]
    row_len = pts_dev * col_count
    col_len = pts_dev * row_count
    col_ratio = col_count // row_count
    all_points = lax.all_gather(points, ("row", "col"), axis=1, tiled=True)
    sq_norms = jnp.sum(all_points * all_points, axis=0)
    row_points = lax.dynamic_slice_in_dim(all_points, row_index * row_len, row_len, 1)
    row_sq = lax.dynamic_slice_in_dim(sq_norms, row_index * row_len, row_len, 0)
    col_points = lax.dynamic_slice_in_dim(all_points, col_index * col_len, col_len, 1)
    col_sq = lax.dynamic_slice_in_dim(sq_norms, col_index * col_len, col_len, 0)
    tile_rows = math.gcd(row_len, 512)
    tile_count = row_len // tile_rows
    rhs_count = right_sides.shape[0]
    residual = right_sides
    solution = jnp.zeros_like(residual)
    direction = residual
    gram = gram_sum(products(residual, residual))
    first = gram
    new_gram = gram
    for iteration in range(ITERS):
        source = lax.dynamic_slice_in_dim(direction, col_index % col_ratio * col_len, col_len, 1)
        col_direction = from_root(source, "row", col_index // col_ratio)

        def one_tile(index, result):
            offset = index * tile_rows
            tile_points = lax.dynamic_slice_in_dim(row_points, offset, tile_rows, 1)
            tile_sq = lax.dynamic_slice_in_dim(row_sq, offset, tile_rows, 0)
            sq_dist = (
                tile_sq[:, None]
                + col_sq[None, :]
                - 2.0 * jnp.dot(tile_points.T, col_points, precision=HIGH)
            )
            kernel = jnp.exp(-0.5 * sq_dist)
            return lax.dynamic_update_slice_in_dim(
                result, products(col_direction, kernel), offset, 1
            )

        image = (
            lax.psum(
                lax.fori_loop(
                    0, tile_count, one_tile, jnp.zeros((rhs_count, row_len), jnp.float32)
                ),
                "col",
            )
            + noise_level[None, :] * direction
        )
        curv, cross, image_gram = triple_sum(
            products(direction, image), products(residual, image), products(image, image)
        )
        step_coef = solve_sym(curv, gram)
        solution = solution + jnp.dot(step_coef.T, direction, precision=HIGH)
        residual = residual - jnp.dot(step_coef.T, image, precision=HIGH)
        cross_coef = jnp.dot(cross, step_coef, precision=HIGH)
        quad = jnp.dot(step_coef.T, jnp.dot(image_gram, step_coef, precision=HIGH), precision=HIGH)
        new_gram = gram - cross_coef - cross_coef.T + quad
        if iteration + 1 < ITERS:
            dir_coef = solve_sym(gram, new_gram)
            direction = residual + jnp.dot(dir_coef.T, direction, precision=HIGH)
        gram = new_gram
    rel_norms = jnp.sqrt(jnp.diagonal(new_gram) / jnp.diagonal(first))
    return (solution, residual, rel_norms)


def solution(mesh):
    placed = (P(None, ("row", "col")), P("row"), P(None, "row"))
    return jax.shard_map(
        on_device,
        mesh=mesh,
        in_specs=placed,
        out_specs=(P(None, "row"), P(None, "row"), P()),
        check_vma=False,
    )
```
